32 devices in a mesh: pipe: 4 (over x, core), exp: 4 (over z), pair: 2 (over y).
Axes of the slice: x: 2, y: 2, z: 4, core: 2. Of those that a mesh axis runs over, the one named last changes fastest.
Arguments:
- hidden_in: bfloat16 [4, 256, 2048], P(None, ('exp', 'pair')), may hold values from -6 to 6
- routes: int32 [4, 4, 256, 8], P('pipe', None, ('exp', 'pair')), may hold values from 0 to 15, all different within a row; in each aligned block of 32 rows (0 to 31, 32 to 63, ..., all dimensions but the last counted through in order) at most 24 rows name the same one
- gate_probs: float32 [4, 4, 256, 8], P('pipe', None, ('exp', 'pair')), may hold values from 0.02 to 1
- norm_gain: float32 [4, 2048], P('pipe'), may hold values from 0.1 to 1.9
- w_gate: bfloat16 [4, 16, 2048, 768], P('pipe', ('exp', 'pair')), may hold values from -0.125 to 0.125
- w_up: bfloat16 [4, 16, 2048, 768], P('pipe', ('exp', 'pair')), may hold values from -0.125 to 0.125
- w_down: bfloat16 [4, 16, 768, 2048], P('pipe', ('exp', 'pair')), may hold values from -0.21875 to 0.21875
Outputs:
- layer_outputs: bfloat16 [4, 4, 256, 2048], P('pipe', None, ('exp', 'pair'))
The draws below stay inside these ranges and needn't reach their ends.
Inputs may be any that keep to these rules, and one draw needn't show every extreme that they name: `routes`: within each layer and micro-batch, the 32 tokens of one device (aligned blocks) name no expert more than 24 times in all, and each token names 8 different experts.
All inputs are finite; a program needn't handle non-finite values.
Results may differ from the reference program's by a relative error of at most 0.01.
Values may be sent and summed in bfloat16 or wider, within the bound.
A program may use at most 64 MiB of HBM per device.

```python
import math
import jax
import jax.numpy as jnp
import numpy as np
from jax import lax

D = 2048
FF = 768
TOPK = 8
MB = 4
TOK_DEV = 32
EXPERTS = 16
LAYERS = 4
TOKENS = 256
CAP = 24


def block_scale(rng, shape, shards, least, largest):
    def one(position, parts):
        steps = jax.random.uniform(jax.random.fold_in(jax.random.fold_in(rng, 6), position), (parts,), jnp.float32, least / len(shards), largest / len(shards))
        return jnp.repeat(jnp.exp(steps), shape[position] // parts).reshape((-1,) + (1,) * (len(shape) - position - 1))

    loudness = one(*shards[0])
    for cut in shards[1:]:
        loudness = loudness * one(*cut)
    return loudness


def routed_block(rng, own, number, rows, number_of, top, bound, skew):
    order = jax.random.permutation(rng, number_of)
    packed, common = shares(number_of, rows * top, bound, skew, True), shares(number_of, rows * top, bound, skew, False)
    places = jnp.arange(number_of)

    def named(sizes, rotation):
        used = int((sizes > 0).sum())
        fixed = max(1, used // 4)
        shifted = fixed + (places - fixed + rotation * (used - fixed)) % max(1, number_of - fixed)
        return jnp.zeros((number_of,), jnp.int32).at[order[jnp.where(places < fixed, places, shifted)]].set(jnp.asarray(sizes, jnp.int32))

    sizes = jnp.where(number % 4 == 0, named(packed, number // 4), named(common, number - number // 4 - 1))
    mixed = jax.random.permutation(jax.random.fold_in(own, 3), number_of)
    donor, taker = mixed[0:number_of // 2 * 2:2], mixed[1:number_of // 2 * 2:2]
    margin = jnp.minimum(sizes[donor] - 1, bound - sizes[taker]) // 2
    margin = jnp.where((donor == order[0]) | (taker == order[0]) | (sizes[taker] == 0), 0, jnp.maximum(margin, 0))
    shifted = jax.random.randint(jax.random.fold_in(own, 4), (number_of // 2,), 0, 1 << 20) % (margin + 1)
    sizes = sizes.at[donor].add(-shifted).at[taker].add(shifted)
    labels = jnp.searchsorted(jnp.cumsum(sizes), jnp.arange(rows * top), side="right").astype(jnp.int32)
    grid = labels.reshape(top, rows).T
    grid = grid[jax.random.permutation(jax.random.fold_in(own, 1), rows)]
    rotation = jax.random.randint(jax.random.fold_in(own, 2), (rows, 1), 0, top)
    return jnp.take_along_axis(grid, (jnp.arange(top)[None, :] + rotation) % top, axis=1)


def shares(number_of, total, most, skew, full):
    loads = [(1 << 20) // math.isqrt(grade ** skew) + 1 for grade in range(1, number_of + 1)]
    largest = most if full else min(most, max(-(-total // number_of), total * loads[0] // sum(loads)))
    least = 1 if total - largest >= number_of - 1 else 0
    counts, surplus = [largest] + [least] * (number_of - 1), total - largest - least * (number_of - 1)
    while surplus > 0:
        candidates = [i for i in range(1, number_of) if counts[i] < largest] or [i for i in range(1, number_of) if counts[i] < most]
        mass, remaining = sum([loads[i] for i in candidates]), surplus
        for i in candidates:
            addition = min(most - counts[i], max(1, remaining * loads[i] // mass), surplus)
            counts[i] = counts[i] + addition
            surplus = surplus - addition
    return np.array(counts)


def normal_values(own_key, dims, width, most, shards=(), held_as=jnp.bfloat16):
    drawn = jax.random.normal(own_key, dims, jnp.float32) * width
    if len(shards) > 0:
        drawn = block_scale(own_key, dims, shards, -0.22, 0.18) * drawn
    return jnp.clip(drawn, min=-most, max=most).astype(held_as)


def setup_inputs(seed: int = 0) -> dict:
    key_of = jax.random.split(jax.random.key(seed), 8)
    hidden_in = normal_values(key_of[0], (MB, TOKENS, D), 1.0, 6.0, ((1, 8),))
    routes_keys = jax.random.split(jax.random.fold_in(key_of[1], 1), LAYERS * MB * TOKENS // TOK_DEV)
    routes_turns = jax.random.permutation(jax.random.fold_in(key_of[1], 3), LAYERS * MB * TOKENS // TOK_DEV)
    routes = jax.vmap(lambda own, number: routed_block(jax.random.fold_in(key_of[1], 2), own, number, TOK_DEV, EXPERTS, TOPK, CAP, 2))(routes_keys, routes_turns).reshape((LAYERS, MB, TOKENS, TOPK))
    gate_probs = jnp.clip(jnp.exp(math.log(1.0) - 3.912023 * jax.random.uniform(key_of[2], (LAYERS, MB, TOKENS, TOPK), jnp.float32) ** block_scale(key_of[2], (LAYERS, MB, TOKENS, TOPK), ((0, 4), (2, 8)), -0.2, 0.2)), 0.02, 1.0)
    norm_gain = jnp.clip(1.0 + 0.18 * jax.random.normal(key_of[3], (LAYERS, D), jnp.float32), 0.1, 1.9)
    w_gate = normal_values(key_of[4], (LAYERS, EXPERTS, D, FF), D ** -0.5, 0.125, ((0, 4), (1, 8)))
    w_up = normal_values(key_of[5], (LAYERS, EXPERTS, D, FF), D ** -0.5, 0.125, ((0, 4), (1, 8)))
    w_down = normal_values(key_of[6], (LAYERS, EXPERTS, FF, D), FF ** -0.5, 0.21875, ((0, 4), (1, 8)))
    return {"hidden_in": hidden_in, "routes": routes, "gate_probs": gate_probs, "norm_gain": norm_gain, "w_gate": w_gate, "w_up": w_up, "w_down": w_down}


EPS = 1e-06

def slots_of(block_routes):
    expert_ids = jnp.arange(EXPERTS, dtype=jnp.int32)
    onehot = (block_routes[:, None] == expert_ids[None, :]).astype(jnp.int32)
    before = jnp.cumsum(onehot, axis=0) - onehot
    return lax.optimization_barrier(jnp.sum(before * onehot, axis=1)).astype(jnp.int32)

def moe_layer(state, chosen, probs, gain, wgate, wupper, wdown):
    floated = state.astype(jnp.float32)
    scale = lax.rsqrt(lax.optimization_barrier(jnp.mean(floated * floated, axis=-1, keepdims=True)) + EPS)
    normed = (floated * scale * gain.astype(jnp.float32)).astype(jnp.bfloat16)
    blocks = TOKENS // TOK_DEV
    flat_routes = chosen.reshape(blocks, TOK_DEV * TOPK).astype(jnp.int32)
    slots = jax.vmap(slots_of)(flat_routes)
    columns = (slots + CAP * jnp.arange(blocks, dtype=jnp.int32)[:, None]).reshape(-1)
    rows_ids = flat_routes.reshape(-1)
    buffer = jnp.zeros((EXPERTS, blocks * CAP, D), jnp.bfloat16)
    buffer = buffer.at[rows_ids, columns].set(jnp.repeat(normed, TOPK, axis=0))

    def one_expert(items):
        inputs, gate_w, up_w, down_w = items
        gate = jnp.dot(inputs, gate_w, preferred_element_type=jnp.float32)
        upward = jnp.dot(inputs, up_w, preferred_element_type=jnp.float32)
        hidden = (jax.nn.silu(gate) * upward).astype(jnp.bfloat16)
        return jnp.dot(hidden, down_w, preferred_element_type=jnp.float32).astype(jnp.bfloat16)
    produced = lax.map(one_expert, (buffer, wgate, wupper, wdown))
    picked = produced[rows_ids, columns].reshape(TOKENS, TOPK, D).astype(jnp.float32)
    probs32 = probs.astype(jnp.float32)
    weights = probs32 / lax.optimization_barrier(jnp.sum(probs32, axis=-1, keepdims=True))
    mixed = jnp.einsum('tk,tkd->td', weights, picked)
    return (floated + mixed).astype(jnp.bfloat16)

def reference(hidden_in, routes, gate_probs, norm_gain, w_gate, w_up, w_down):
    current = hidden_in
    outputs = []
    for layer in range(LAYERS):

        def per_batch(items):
            state, chosen, probs = items
            return moe_layer(state, chosen, probs, norm_gain[layer], w_gate[layer], w_up[layer], w_down[layer])
        current = lax.map(per_batch, (current, routes[layer], gate_probs[layer]))
        outputs.append(current)
    return jnp.stack(outputs, axis=0)
```

```python
import functools

import jax
import jax.numpy as jnp
from jax import lax
from jax.experimental import pallas as pl
from jax.experimental.pallas import tpu as pltpu
from jax.sharding import PartitionSpec as P

EPS = 1e-06
MESH = pl.DeviceIdType.MESH
F32 = jnp.float32
BF16 = jnp.bfloat16
PIECES = 2
AHEAD = 2
RELAY_AHEAD = 2
LOCAL = 1
SPARE = 5
SCHEDULE = (
    (("C", 0, 0, 99), ("S", 0, 0, 99), ("E", 0, 0, 99), ("A", 0, 0, 99), ("F", 1, 0, 99)),
    (("C", 0, 0, 99), ("S", 0, 0, 99), ("F", 1, 0, 99), ("E", 0, 0, 99)),
    (("C", 0, 0, 99), ("F", 1, 0, 99), ("E", -1, 0, 99), ("S", 0, 0, 99)),
    (("C", 0, 0, 99), ("F", 1, 0, 99), ("E", -1, 0, 99), ("S", 0, 0, 99)),
)
VMEM_LIMIT = 63 * 1024 * 1024


def divisor_tile(size, most):
    tile = most
    while size % tile:
        tile //= 2
    return tile


def relay_kernel(
    stages,
    zs,
    ys,
    hidden_ref,
    routes_ref,
    probs_ref,
    gain_ref,
    wgate_ref,
    wup_ref,
    wdown_ref,
    out_ref,
    wg,
    wu,
    wd,
    hbuf,
    tokens,
    share,
    column,
    hid,
    part,
    fromy,
    zsend,
    fromz,
    obuf,
    nbuf,
    gnext,
    relay,
    gfirst,
    w_sem,
    h_sem,
    hs_sem,
    o_sem,
    s_sem,
    sr_sem,
    a_sem,
    ar_sem,
    f_sem,
    y_sem,
    yr_sem,
    z_sem,
    zr_sem,
    g_sem,
    gr_sem,
    hr_sem,
    b_sem,
    rr_sem,
    q_sem,
    v_sem,
):
    micro, rows, width = hbuf.shape
    locals_, _, ff = wg.shape
    span = share.shape[2]
    groups = zs * ys
    experts = groups * locals_
    stage = lax.axis_index("pipe")
    z = lax.axis_index("exp")
    y = lax.axis_index("pair")
    me = z * ys + y
    slot = y * zs + z
    upper_half = lax.div(2 * z, zs)
    turn = 1 - 2 * upper_half
    is_first = stage == 0
    has_last = stage > 0
    has_next = stage < stages - 1
    helper = stages // 2
    local = min(LOCAL, micro) if helper else micro
    is_helper = jnp.logical_and(stage == helper, stage > 0)

    def block(at):
        return pl.ds(pl.multiple_of(at * rows, rows), rows)

    def along(k):
        return lax.rem(z + turn * k + zs, zs)

    def across(dy):
        return lax.rem(y + dy, ys)

    def peer(dz, dy):
        return lax.rem(z + dz, zs), lax.rem(y + dy, ys)

    others = [(dz, dy) for dy in range(ys) for dz in range(zs) if dz or dy]

    loads = []
    for j in range(locals_):
        loads.append(
            (
                pltpu.make_async_copy(wgate_ref.at[0, j], wg.at[j], w_sem.at[3 * j]),
                pltpu.make_async_copy(wup_ref.at[0, j], wu.at[j], w_sem.at[3 * j + 1]),
                pltpu.make_async_copy(
                    wdown_ref.at[0, j], wd.at[pl.ds(j * ff, ff)], w_sem.at[3 * j + 2]
                ),
            )
        )

    def from_input(m):
        return pltpu.make_async_copy(hidden_ref.at[m], hbuf.at[m], h_sem.at[m])

    @pl.when(is_first)
    def _():
        for m in range(micro):
            from_input(m).start()

    def relay_input(m):
        here = relay.at[m, block(slot)]
        return pltpu.make_async_copy(hidden_ref.at[m], here, hr_sem.at[m])

    @pl.when(is_helper)
    def _():
        for m in range(local, micro):
            relay_input(m).start()

    for j in range(locals_):
        loads[j][0].start()
        loads[j][1].start()
    for j in range(locals_):
        loads[j][2].start()

    barrier = pltpu.get_barrier_semaphore()
    for dz, dy in others:
        pz, py = peer(dz, dy)
        pl.semaphore_signal(barrier, inc=1, device_id={"exp": pz, "pair": py}, device_id_type=MESH)

    @pl.when(has_last)
    def _():
        for k in range(zs):
            pl.semaphore_signal(
                barrier,
                inc=1,
                device_id={"pipe": stage - 1, "exp": along(k)},
                device_id_type=MESH,
            )

    @pl.when(has_next)
    def _():
        for k in range(zs):
            pl.semaphore_signal(
                barrier,
                inc=1,
                device_id={"pipe": stage + 1, "exp": along(k)},
                device_id_type=MESH,
            )

    if local < micro:

        @pl.when(is_first)
        def _():
            pl.semaphore_signal(
                barrier, inc=1, device_id={"pipe": helper}, device_id_type=MESH
            )

        @pl.when(is_helper)
        def _():
            pl.semaphore_signal(barrier, inc=1, device_id={"pipe": 0}, device_id_type=MESH)

    batches, top, held_rows = routes_ref.shape[1:]
    named_ids = lax.broadcasted_iota(jnp.int32, (experts, held_rows), 0)
    for m in range(batches):
        probs = probs_ref[0, m]
        normal = probs / jnp.sum(probs, axis=0, keepdims=True)
        chosen = routes_ref[0, m]
        total = jnp.zeros((experts, held_rows), F32)
        for k in range(top):
            total = total + jnp.where(
                named_ids == chosen[k : k + 1], normal[k : k + 1], 0.0
            )
        share[slot, :, m * held_rows : (m + 1) * held_rows] = total

    linked = has_last.astype(jnp.int32) + has_next.astype(jnp.int32)
    awaited = len(others) + linked * zs
    if local < micro:
        awaited = awaited + is_first.astype(jnp.int32) + is_helper.astype(jnp.int32)
    pl.semaphore_wait(barrier, awaited)

    def share_copy(at, to_z, to_y):
        return pltpu.make_async_remote_copy(
            src_ref=share.at[at],
            dst_ref=share.at[at],
            send_sem=s_sem.at[to_y * zs + to_z],
            recv_sem=sr_sem.at[at],
            device_id={"exp": to_z, "pair": to_y},
            device_id_type=MESH,
        )

    def share_send():
        for dz, dy in others:
            pz, py = peer(dz, dy)
            share_copy(slot, pz, py).start()

    def share_wait():
        for dz, dy in others:
            pz, py = peer(dz, dy)
            share_copy(py * zs + pz, pz, py).wait_recv()

    def gain_copy():
        return pltpu.make_async_remote_copy(
            src_ref=gain_ref,
            dst_ref=gnext,
            send_sem=g_sem.at[0],
            recv_sem=gr_sem.at[0],
            device_id={"pipe": stage - 1},
            device_id_type=MESH,
        )

    def first_gain_copy():
        return pltpu.make_async_remote_copy(
            src_ref=gain_ref,
            dst_ref=gfirst,
            send_sem=g_sem.at[1],
            recv_sem=gr_sem.at[1],
            device_id={"pipe": helper},
            device_id_type=MESH,
        )

    def relay_z(m, k):
        here = relay.at[m, block(slot)]
        return pltpu.make_async_remote_copy(
            src_ref=here,
            dst_ref=here,
            send_sem=b_sem.at[m, k],
            recv_sem=rr_sem.at[m, slot],
            device_id={"exp": along(k)},
            device_id_type=MESH,
        )

    def relay_y(m, at, dz, dy):
        here = relay.at[m, block(at)]
        return pltpu.make_async_remote_copy(
            src_ref=here,
            dst_ref=here,
            send_sem=q_sem.at[m, dz * max(1, ys - 1) + dy - 1],
            recv_sem=rr_sem.at[m, at],
            device_id={"pair": across(dy)},
            device_id_type=MESH,
        )

    def relay_x(m, at):
        return pltpu.make_async_remote_copy(
            src_ref=relay.at[m, block(at)],
            dst_ref=tokens.at[m, block(at)],
            send_sem=v_sem.at[m, at],
            recv_sem=ar_sem.at[m, at],
            device_id={"pipe": 0},
            device_id_type=MESH,
        )

    def z_token(m, k):
        here = tokens.at[m, block(slot)]
        return pltpu.make_async_remote_copy(
            src_ref=here,
            dst_ref=here,
            send_sem=a_sem.at[m, k],
            recv_sem=ar_sem.at[m, slot],
            device_id={"exp": along(k)},
            device_id_type=MESH,
        )

    def next_token(m, k):
        return pltpu.make_async_remote_copy(
            src_ref=nbuf.at[m],
            dst_ref=tokens.at[m, block(slot)],
            send_sem=a_sem.at[m, k],
            recv_sem=ar_sem.at[m, slot],
            device_id={"pipe": stage + 1, "exp": along(k)},
            device_id_type=MESH,
        )

    def y_token(m, at, dz, dy):
        here = tokens.at[m, block(at)]
        return pltpu.make_async_remote_copy(
            src_ref=here,
            dst_ref=here,
            send_sem=f_sem.at[m, dz * max(1, ys - 1) + dy - 1],
            recv_sem=ar_sem.at[m, at],
            device_id={"pair": across(dy)},
            device_id_type=MESH,
        )

    def y_copy(m, dy, tz):
        return pltpu.make_async_remote_copy(
            src_ref=part.at[m, block(across(dy) * zs + tz)],
            dst_ref=fromy.at[m, dy - 1, tz],
            send_sem=y_sem.at[m, dy - 1, tz],
            recv_sem=yr_sem.at[m, dy - 1, tz],
            device_id={"pair": across(dy)},
            device_id_type=MESH,
        )

    def z_copy(m, k, source):
        return pltpu.make_async_remote_copy(
            src_ref=zsend.at[m, k],
            dst_ref=fromz.at[m, source],
            send_sem=z_sem.at[m, k - 1],
            recv_sem=zr_sem.at[m, source],
            device_id={"exp": along(k)},
            device_id_type=MESH,
        )

    def hand_copy(m):
        return pltpu.make_async_remote_copy(
            src_ref=obuf.at[m],
            dst_ref=hbuf.at[m],
            send_sem=hs_sem.at[m],
            recv_sem=h_sem.at[m],
            device_id={"pipe": stage + 1},
            device_id_type=MESH,
        )

    def out_copy(m):
        return pltpu.make_async_copy(obuf.at[m], out_ref.at[0, m], o_sem.at[m])

    def normed(state, gain):
        scale = lax.rsqrt(jnp.mean(state * state, axis=-1, keepdims=True) + EPS)
        return (state * scale * gain[...]).astype(BF16)

    def announce(m):
        from_input(m).wait()
        tokens[m, block(slot)] = normed(hbuf[m].astype(F32), gain_ref)
        for k in range(zs - 1, 0, -1):
            z_token(m, k).start()

    def relay_announce(m):
        relay_input(m).wait()
        relay[m, block(slot)] = normed(relay[m, block(slot)].astype(F32), gfirst)
        for k in range(zs - 1, 0, -1):
            relay_z(m, k).start()

    def relay_near(m):
        for dz in range(zs):
            at = y * zs + along(dz)
            if dz:
                relay_y(m, at, dz, 0).wait_recv()
            for dy in range(1, ys):
                relay_y(m, at, dz, dy).start()
            relay_x(m, at).start()

    def relay_far(m):
        for dy in range(1, ys):
            for dz in range(zs):
                at = across(dy) * zs + along(dz)
                relay_y(m, at, dz, dy).wait_recv()
                relay_x(m, at).start()

    def forward(m):
        for dz in range(zs):
            at = y * zs + along(dz)
            if dz:
                y_token(m, at, dz, 0).wait_recv()
            else:

                @pl.when(has_last)
                def _():
                    y_token(m, at, dz, 0).wait_recv()

            for dy in range(1, ys):
                y_token(m, at, dz, dy).start()

    def arrive(m):
        @pl.when(jnp.logical_and(is_first, m >= local))
        def _():
            for dz in range(zs):
                relay_x(m, y * zs + along(dz)).wait_recv()

        for dy in range(1, ys):
            for dz in range(zs):
                y_token(m, across(dy) * zs + along(dz), dz, dy).wait_recv()

    ftile = divisor_tile(ff, 256)
    ntile = divisor_tile(width, 512)
    count = groups * rows

    def spread():
        ids = lax.broadcasted_iota(jnp.int32, (groups, experts, span), 1)
        held = share[...]
        mine = [
            jnp.sum(jnp.where(ids == me * locals_ + j, held, 0.0), axis=1)
            for j in range(locals_)
        ]
        padding = jnp.zeros((128 - locals_ * groups, span), F32)
        column[...] = jnp.transpose(jnp.concatenate(mine + [padding], axis=0))

    def upper(m):
        weights = column[pl.ds(pl.multiple_of(m * rows, rows), rows)]
        for j in range(locals_):
            scaled = jnp.concatenate(
                [weights[:, j * groups + g : j * groups + g + 1] for g in range(groups)], axis=0
            )

            @pl.when(m == 0)
            def _():
                loads[j][0].wait()
                loads[j][1].wait()

            for c in range(0, ff, ftile):
                held = tokens[m]
                gate = jnp.dot(held, wg[j, :, c : c + ftile], preferred_element_type=F32)
                upward = jnp.dot(held, wu[j, :, c : c + ftile], preferred_element_type=F32)
                hid[:, j * ff + c : j * ff + c + ftile] = (
                    jax.nn.silu(gate) * upward * scaled
                ).astype(BF16)

    def lower(m):
        @pl.when(m == 0)
        def _():
            for j in range(locals_):
                loads[j][2].wait()

        for c in range(0, width, ntile):
            part[m, :, c : c + ntile] = jnp.dot(
                hid[...], wd[:, c : c + ntile], preferred_element_type=F32
            ).astype(BF16)

    def compute(m):
        arrive(m)
        upper(m)
        lower(m)
        for dy in range(1, ys):
            for k in range(zs - 1, -1, -1):
                y_copy(m, dy, along(k)).start()

    def own_part(m, pz):
        return part[m, block(y * zs + pz)].astype(F32)

    def scatter(m):
        for k in range(zs - 1, 0, -1):
            pz = along(k)
            total = own_part(m, pz)
            for dy in range(1, ys):
                y_copy(m, dy, pz).wait_recv()
                total = total + fromy[m, dy - 1, pz].astype(F32)
            zsend[m, k] = total.astype(BF16)
            z_copy(m, k, z).start()

    def finish(m):
        @pl.when(jnp.logical_or(has_last, m >= local))
        def _():
            from_input(m).wait()

        total = hbuf[m].astype(F32) + own_part(m, z)
        for dy in range(1, ys):
            y_copy(m, dy, z).wait_recv()
            total = total + fromy[m, dy - 1, z].astype(F32)
        for k in range(1, zs):
            z_copy(m, k, along(k)).wait_recv()
            total = total + fromz[m, along(k)].astype(F32)
        state = total.astype(BF16)
        obuf[m] = state

        @pl.when(has_next)
        def _():
            nbuf[m] = normed(state.astype(F32), gnext)
            for k in range(zs - 1, -1, -1):
                next_token(m, k).start()
            hand_copy(m).start()

        out_copy(m).start()

    @pl.when(is_first)
    def _():
        if local < micro:
            first_gain_copy().start()
        for m in range(min(AHEAD, local)):
            announce(m)

    @pl.when(has_last)
    def _():
        gain_copy().start()

    share_send()

    @pl.when(is_helper)
    def _():
        if local < micro:
            first_gain_copy().wait_recv()
            for m in range(local, min(micro, local + RELAY_AHEAD)):
                relay_announce(m)

            @pl.loop(local, micro + 1)
            def _(m):
                @pl.when(m < micro)
                def _():
                    relay_near(m)

                @pl.when(m + RELAY_AHEAD < micro)
                def _():
                    relay_announce(m + RELAY_AHEAD)

                @pl.when(m > local)
                def _():
                    relay_far(m - 1)

    @pl.when(has_next)
    def _():
        gain_copy().wait_recv()

    share_wait()
    spread()
    handlers = {"A": announce, "F": forward, "S": scatter, "E": finish}
    centre = [[item[0] for item in listed].index("C") for listed in SCHEDULE]

    def serve(step, late):
        for at, listed in enumerate(SCHEDULE[:stages]):
            items = listed[centre[at] + 1 :] if late else listed[: centre[at]]
            mine = stage == at if at + 1 < len(SCHEDULE) else stage >= at

            @pl.when(mine)
            def _():
                for name, lead, low, high in items:
                    m = step + lead
                    if name in "AF" and at == 0:
                        high = min(high, local)
                    if name == "A":
                        low = max(low, AHEAD)
                    if low >= min(high, micro):
                        continue

                    @pl.when(jnp.logical_and(m >= low, m < min(high, micro)))
                    def _():
                        handlers[name](m)

    @pl.loop(0, micro + SPARE)
    def _(turn_number):
        step = turn_number - 1
        serve(step, False)

        @pl.when(jnp.logical_and(step >= 0, step < micro))
        def _():
            compute(step)

        serve(step, True)

    for dz, dy in others:
        pz, py = peer(dz, dy)
        share_copy(slot, pz, py).wait_send()

    @pl.when(has_last)
    def _():
        gain_copy().wait_send()

    if local < micro:

        @pl.when(is_first)
        def _():
            first_gain_copy().wait_send()

        @pl.when(is_helper)
        def _():
            @pl.loop(local, micro)
            def _(m):
                for k in range(1, zs):
                    relay_z(m, k).wait_send()
                for dz in range(zs):
                    for dy in range(1, ys):
                        relay_y(m, slot, dz, dy).wait_send()
                for at in range(groups):
                    relay_x(m, at).wait_send()

    @pl.loop(0, micro)
    def _(m):
        for k in range(1, zs):
            z_copy(m, k, z).wait_send()

        direct = jnp.logical_or(has_last, m < local)

        @pl.when(jnp.logical_and(is_first, direct))
        def _():
            for k in range(1, zs):
                z_token(m, k).wait_send()

        @pl.when(direct)
        def _():
            for dy in range(1, ys):
                for tz in range(zs):
                    y_token(m, slot, tz, dy).wait_send()

        @pl.when(has_next)
        def _():
            for k in range(zs):
                next_token(m, k).wait_send()
            hand_copy(m).wait_send()

        for dy in range(1, ys):
            for tz in range(zs):
                y_copy(m, dy, tz).wait_send()

        out_copy(m).wait()


def relayed(hidden_in, routes, gate_probs, norm_gain, w_gate, w_up, w_down):
    batches, whole_rows, _ = hidden_in.shape
    pieces = PIECES if whole_rows % (16 * PIECES) == 0 else 1
    hidden_in = cut(hidden_in, 0, pieces)
    routes = jnp.transpose(routes, (0, 1, 3, 2))
    gate_probs = jnp.transpose(gate_probs, (0, 1, 3, 2))
    micro, rows, width = hidden_in.shape
    _, locals_, _, ff = w_gate.shape
    stages, zs, ys = (lax.axis_size(a) for a in ("pipe", "exp", "pair"))
    groups = zs * ys
    dma = pltpu.SemaphoreType.DMA
    anywhere = pl.BlockSpec(memory_space=pl.ANY)
    inside = pl.BlockSpec(memory_space=pltpu.VMEM)
    out = pl.pallas_call(
        functools.partial(relay_kernel, stages, zs, ys),
        out_shape=jax.ShapeDtypeStruct((1, micro, rows, width), BF16),
        in_specs=[anywhere, inside, inside, inside, anywhere, anywhere, anywhere],
        out_specs=anywhere,
        scratch_shapes=[
            pltpu.VMEM((locals_, width, ff), BF16),
            pltpu.VMEM((locals_, width, ff), BF16),
            pltpu.VMEM((locals_ * ff, width), BF16),
            pltpu.VMEM((micro, rows, width), BF16),
            pltpu.VMEM((micro, groups * rows, width), BF16),
            pltpu.VMEM((groups, groups * locals_, micro * rows), F32),
            pltpu.VMEM((micro * rows, 128), F32),
            pltpu.VMEM((groups * rows, locals_ * ff), BF16),
            pltpu.VMEM((micro, groups * rows, width), BF16),
            pltpu.VMEM((micro, max(1, ys - 1), zs, rows, width), BF16),
            pltpu.VMEM((micro, zs, rows, width), BF16),
            pltpu.VMEM((micro, zs, rows, width), BF16),
            pltpu.VMEM((micro, rows, width), BF16),
            pltpu.VMEM((micro, rows, width), BF16),
            pltpu.VMEM((1, width), F32),
            pltpu.VMEM((micro, groups * rows, width), BF16),
            pltpu.VMEM((1, width), F32),
            dma((3 * locals_,)),
            dma((micro,)),
            dma((micro,)),
            dma((micro,)),
            dma((groups,)),
            dma((groups,)),
            dma((micro, zs)),
            dma((micro, groups)),
            dma((micro, zs * max(1, ys - 1))),
            dma((micro, max(1, ys - 1), zs)),
            dma((micro, max(1, ys - 1), zs)),
            dma((micro, max(1, zs - 1))),
            dma((micro, zs)),
            dma((2,)),
            dma((2,)),
            dma((micro,)),
            dma((micro, zs)),
            dma((micro, groups)),
            dma((micro, zs * max(1, ys - 1))),
            dma((micro, groups)),
        ],
        compiler_params=pltpu.CompilerParams(
            collective_id=0, has_side_effects=True, vmem_limit_bytes=VMEM_LIMIT
        ),
    )(hidden_in, routes, gate_probs, norm_gain, w_gate, w_up, w_down)
    return out.reshape(1, batches, whole_rows, width)


def cut(value, axis, pieces):
    shape = value.shape
    rows = shape[axis + 1] // pieces
    return value.reshape(shape[:axis] + (shape[axis] * pieces, rows) + shape[axis + 2 :])


def kernel_fits(hidden_in, w_gate, groups):
    micro, rows, width = hidden_in.shape
    _, locals_, _, ff = w_gate.shape
    weights = 3 * locals_ * width * ff
    moved = micro * rows * width * (5 * groups + 6)
    small = groups * rows * (locals_ * ff + 2 * micro * groups * locals_)
    fits = 2 * (weights + moved + small) + 8 * 1024 * 1024 < VMEM_LIMIT
    small_enough = groups * locals_ <= 128 and micro * rows % 128 == 0
    return fits and small_enough and rows % 16 == 0 and width % 128 == 0 and ff % 128 == 0


def passed_along(value, axis, steps):
    count = lax.axis_size(axis)
    first, last = (max(0, -steps), min(count, count - steps))
    return lax.ppermute(value, axis, [(source, source + steps) for source in range(first, last)])


def expert_block(arrived, wgate, wupper, wdown):
    gate = jnp.einsum("nlcd,ldf->nlcf", arrived, wgate, preferred_element_type=jnp.float32)
    upward = jnp.einsum("nlcd,ldf->nlcf", arrived, wupper, preferred_element_type=jnp.float32)
    hidden = (jax.nn.silu(gate) * upward).astype(jnp.bfloat16)
    return jnp.einsum("nlcf,lfd->nlcd", hidden, wdown, preferred_element_type=jnp.float32).astype(
        jnp.bfloat16
    )


def on_device(hidden_in, routes, gate_probs, norm_gain, w_gate, w_up, w_down):
    if kernel_fits(hidden_in, w_gate, lax.axis_size(("exp", "pair"))):
        return relayed(hidden_in, routes, gate_probs, norm_gain, w_gate, w_up, w_down)
    section = lax.axis_index("pipe")
    micro, tok_rows, width = hidden_in.shape
    top_count = routes.shape[3]
    groups = lax.axis_size(("exp", "pair"))
    local_experts = w_gate.shape[1]
    experts = local_experts * groups
    capacity = max(2, 3 * tok_rows * top_count // (2 * experts))
    gain = norm_gain[0]
    wgate = w_gate[0]
    wupper = w_up[0]
    wdown = w_down[0]
    expert_ids = jnp.arange(experts, dtype=jnp.int32)

    def layer(state, index):
        chosen = lax.dynamic_index_in_dim(routes[0], index, 0, keepdims=False).reshape(-1)
        probs = lax.dynamic_index_in_dim(gate_probs[0], index, 0, keepdims=False)
        floated = state.astype(jnp.float32)
        scale = lax.rsqrt(jnp.mean(floated * floated, axis=-1, keepdims=True) + EPS)
        normed = (floated * scale * gain).astype(jnp.bfloat16)
        onehot = (chosen[:, None] == expert_ids[None, :]).astype(jnp.int32)
        before = jnp.cumsum(onehot, axis=0) - onehot
        slots = jnp.sum(before * onehot, axis=1)
        outgoing = jnp.zeros((experts, capacity, width), jnp.bfloat16)
        outgoing = outgoing.at[chosen, slots].set(jnp.repeat(normed, top_count, axis=0))
        grouped = outgoing.reshape(groups, local_experts, capacity, width)
        produced = expert_block(
            lax.all_to_all(grouped, ("exp", "pair"), split_axis=0, concat_axis=0, tiled=True),
            wgate,
            wupper,
            wdown,
        )
        returned = lax.all_to_all(
            produced, ("exp", "pair"), split_axis=0, concat_axis=0, tiled=True
        )
        results = returned.reshape(experts, capacity, width)[chosen, slots]
        results = results.reshape(tok_rows, top_count, width).astype(jnp.float32)
        weights = probs / jnp.sum(probs, axis=-1, keepdims=True)
        mixed = jnp.einsum("tk,tkd->td", weights, results)
        return (floated + mixed).astype(jnp.bfloat16)

    def advance(step, carry):
        received, saved = carry
        index = step - section
        valid = jnp.logical_and(index >= 0, index < micro)
        clipped = jnp.clip(index, 0, micro - 1)
        first = lax.dynamic_index_in_dim(hidden_in, clipped, 0, keepdims=False)
        state = jnp.where(section == 0, first, received)
        updated = layer(state, clipped)
        saved = jnp.where(valid, lax.dynamic_update_index_in_dim(saved, updated, clipped, 0), saved)
        received = passed_along(updated, "pipe", 1)
        return (received, saved)

    start = (
        jnp.zeros((tok_rows, width), jnp.bfloat16),
        jnp.zeros((micro, tok_rows, width), jnp.bfloat16),
    )
    received, saved = lax.fori_loop(0, micro + lax.axis_size("pipe") - 1, advance, start)
    return saved[None]


def solution(mesh):
    in_specs = (
        P(None, ("exp", "pair"), None),
        P("pipe", None, ("exp", "pair"), None),
        P("pipe", None, ("exp", "pair"), None),
        P("pipe", None),
        P("pipe", ("exp", "pair"), None, None),
        P("pipe", ("exp", "pair"), None, None),
        P("pipe", ("exp", "pair"), None, None),
    )
    out_specs = P("pipe", None, ("exp", "pair"), None)
    return jax.shard_map(
        on_device, mesh=mesh, in_specs=in_specs, out_specs=out_specs, check_vma=False
    )
```

```python
import functools

import jax
import jax.numpy as jnp
from jax import lax
from jax.experimental import pallas as pl
from jax.experimental.pallas import tpu as pltpu
from jax.sharding import PartitionSpec as P

EPS = 1e-06
MESH = pl.DeviceIdType.MESH
F32 = jnp.float32
BF16 = jnp.bfloat16
PIECES = 2
RELAY_AHEAD = 2
LOCAL = 2
SCHEDULE = (
    ("FF", "", "S", "SE", "E", "SSS", "EEE", "S", "SEESE"),
    ("FF", "", "SFEFS", "ES", "EFS", "ESFEF", "S", "EFSE", "SE"),
    ("F", "FS", "ESFFE", "", "FSSFE", "", "FSEEF", "S", "SESEE"),
    ("F", "SF", "SF", "FESFE", "FE", "F", "SFS", "SEE", "SSEEE"),
)
VMEM_LIMIT = 63 * 1024 * 1024


def divisor_tile(size, most):
    tile = most
    while size % tile:
        tile //= 2
    return tile


def merged(one, two):
    best = {(len(one), len(two)): ""}
    for i in range(len(one), -1, -1):
        for j in range(len(two), -1, -1):
            options = []
            if i < len(one) and j < len(two) and one[i] == two[j]:
                options.append(one[i] + best[i + 1, j + 1])
            if i < len(one):
                options.append(one[i] + best[i + 1, j])
            if j < len(two):
                options.append(two[j] + best[i, j + 1])
            if options:
                best[i, j] = min(options, key=len)
    return best[0, 0]


def plan_of(stages, micro, local):
    tuned = len(SCHEDULE) == stages and len(SCHEDULE[0]) == micro + 1 and local == LOCAL
    plans = []
    for at in range(stages):
        if tuned:
            gaps = SCHEDULE[at]
        elif at == 0:
            gaps = ("F" * local,) + ("SE",) * micro
        else:
            gaps = ("F",) + ("SFE",) * (micro - 1) + ("SE",)
        slots = functools.reduce(merged, gaps)
        tables = [[] for _ in slots]
        counts = {}
        for step, gap in enumerate(gaps):
            place = 0
            for name in gap:
                place = slots.index(name, place)
                tables[place].append((step, counts.get(name, 0)))
                counts[name] = counts.get(name, 0) + 1
                place += 1
        plans.append(list(zip(slots, tables)))
    return plans


def relay_kernel(
    stages,
    zs,
    ys,
    hidden_ref,
    routes_ref,
    probs_ref,
    gain_ref,
    wgate_ref,
    wup_ref,
    wdown_ref,
    out_ref,
    wg,
    wu,
    wd,
    hbuf,
    tokens,
    share,
    column,
    hid,
    part,
    fromy,
    zsend,
    fromz,
    obuf,
    nbuf,
    gnext,
    relay,
    gfirst,
    w_sem,
    h_sem,
    hs_sem,
    o_sem,
    s_sem,
    sr_sem,
    a_sem,
    ar_sem,
    f_sem,
    y_sem,
    yr_sem,
    z_sem,
    zr_sem,
    g_sem,
    gr_sem,
    hr_sem,
    b_sem,
    rr_sem,
    q_sem,
    v_sem,
):
    micro, rows, width = hbuf.shape
    locals_, _, ff = wg.shape
    span = share.shape[2]
    groups = zs * ys
    experts = groups * locals_
    stage = lax.axis_index("pipe")
    z = lax.axis_index("exp")
    y = lax.axis_index("pair")
    me = z * ys + y
    slot = y * zs + z
    upper_half = lax.div(2 * z, zs)
    turn = 1 - 2 * upper_half
    is_first = stage == 0
    has_last = stage > 0
    has_next = stage < stages - 1
    helper = stages // 2
    local = min(LOCAL, micro) if helper else micro
    is_helper = jnp.logical_and(stage == helper, stage > 0)

    def block(at):
        return pl.ds(pl.multiple_of(at * rows, rows), rows)

    def along(k):
        return lax.rem(z + turn * k + zs, zs)

    def across(dy):
        return lax.rem(y + dy, ys)

    def peer(dz, dy):
        return lax.rem(z + dz, zs), lax.rem(y + dy, ys)

    others = [(dz, dy) for dy in range(ys) for dz in range(zs) if dz or dy]

    loads = []
    for j in range(locals_):
        loads.append(
            (
                pltpu.make_async_copy(wgate_ref.at[0, j], wg.at[j], w_sem.at[3 * j]),
                pltpu.make_async_copy(wup_ref.at[0, j], wu.at[j], w_sem.at[3 * j + 1]),
                pltpu.make_async_copy(
                    wdown_ref.at[0, j], wd.at[pl.ds(j * ff, ff)], w_sem.at[3 * j + 2]
                ),
            )
        )

    def from_input(m):
        return pltpu.make_async_copy(hidden_ref.at[m], hbuf.at[m], h_sem.at[m])

    @pl.when(is_first)
    def _():
        for m in range(micro):
            from_input(m).start()

    def relay_input(m):
        here = relay.at[m, block(slot)]
        return pltpu.make_async_copy(hidden_ref.at[m], here, hr_sem.at[m])

    @pl.when(is_helper)
    def _():
        for m in range(local, micro):
            relay_input(m).start()

    for j in range(locals_):
        loads[j][0].start()
        loads[j][1].start()
    for j in range(locals_):
        loads[j][2].start()

    barrier = pltpu.get_barrier_semaphore()
    for dz, dy in others:
        pz, py = peer(dz, dy)
        pl.semaphore_signal(barrier, inc=1, device_id={"exp": pz, "pair": py}, device_id_type=MESH)

    @pl.when(has_last)
    def _():
        for k in range(zs):
            pl.semaphore_signal(
                barrier,
                inc=1,
                device_id={"pipe": stage - 1, "exp": along(k)},
                device_id_type=MESH,
            )

    @pl.when(has_next)
    def _():
        for k in range(zs):
            pl.semaphore_signal(
                barrier,
                inc=1,
                device_id={"pipe": stage + 1, "exp": along(k)},
                device_id_type=MESH,
            )

    if local < micro:

        @pl.when(is_first)
        def _():
            pl.semaphore_signal(
                barrier, inc=1, device_id={"pipe": helper}, device_id_type=MESH
            )

        @pl.when(is_helper)
        def _():
            pl.semaphore_signal(barrier, inc=1, device_id={"pipe": 0}, device_id_type=MESH)

    batches, top, held_rows = routes_ref.shape[1:]
    named_ids = lax.broadcasted_iota(jnp.int32, (experts, held_rows), 0)
    for m in range(batches):
        probs = probs_ref[0, m]
        normal = probs / jnp.sum(probs, axis=0, keepdims=True)
        chosen = routes_ref[0, m]
        total = jnp.zeros((experts, held_rows), F32)
        for k in range(top):
            total = total + jnp.where(
                named_ids == chosen[k : k + 1], normal[k : k + 1], 0.0
            )
        share[slot, :, m * held_rows : (m + 1) * held_rows] = total

    linked = has_last.astype(jnp.int32) + has_next.astype(jnp.int32)
    awaited = len(others) + linked * zs
    if local < micro:
        awaited = awaited + is_first.astype(jnp.int32) + is_helper.astype(jnp.int32)
    pl.semaphore_wait(barrier, awaited)

    def share_copy(at, to_z, to_y):
        return pltpu.make_async_remote_copy(
            src_ref=share.at[at],
            dst_ref=share.at[at],
            send_sem=s_sem.at[to_y * zs + to_z],
            recv_sem=sr_sem.at[at],
            device_id={"exp": to_z, "pair": to_y},
            device_id_type=MESH,
        )

    def share_send():
        for dz, dy in others:
            pz, py = peer(dz, dy)
            share_copy(slot, pz, py).start()

    def share_wait():
        for dz, dy in others:
            pz, py = peer(dz, dy)
            share_copy(py * zs + pz, pz, py).wait_recv()

    def gain_copy():
        return pltpu.make_async_remote_copy(
            src_ref=gain_ref,
            dst_ref=gnext,
            send_sem=g_sem.at[0],
            recv_sem=gr_sem.at[0],
            device_id={"pipe": stage - 1},
            device_id_type=MESH,
        )

    def first_gain_copy():
        return pltpu.make_async_remote_copy(
            src_ref=gain_ref,
            dst_ref=gfirst,
            send_sem=g_sem.at[1],
            recv_sem=gr_sem.at[1],
            device_id={"pipe": helper},
            device_id_type=MESH,
        )

    def relay_z(m, k):
        here = relay.at[m, block(slot)]
        return pltpu.make_async_remote_copy(
            src_ref=here,
            dst_ref=here,
            send_sem=b_sem.at[m, k],
            recv_sem=rr_sem.at[m, slot],
            device_id={"exp": along(k)},
            device_id_type=MESH,
        )

    def relay_y(m, at, dz, dy):
        here = relay.at[m, block(at)]
        return pltpu.make_async_remote_copy(
            src_ref=here,
            dst_ref=here,
            send_sem=q_sem.at[m, dz * max(1, ys - 1) + dy - 1],
            recv_sem=rr_sem.at[m, at],
            device_id={"pair": across(dy)},
            device_id_type=MESH,
        )

    def relay_x(m, at):
        return pltpu.make_async_remote_copy(
            src_ref=relay.at[m, block(at)],
            dst_ref=tokens.at[m, block(at)],
            send_sem=v_sem.at[m, at],
            recv_sem=ar_sem.at[m, at],
            device_id={"pipe": 0},
            device_id_type=MESH,
        )

    def z_token(m, k):
        here = tokens.at[m, block(slot)]
        return pltpu.make_async_remote_copy(
            src_ref=here,
            dst_ref=here,
            send_sem=a_sem.at[m, k],
            recv_sem=ar_sem.at[m, slot],
            device_id={"exp": along(k)},
            device_id_type=MESH,
        )

    def next_token(m, k):
        return pltpu.make_async_remote_copy(
            src_ref=nbuf.at[m],
            dst_ref=tokens.at[m, block(slot)],
            send_sem=a_sem.at[m, k],
            recv_sem=ar_sem.at[m, slot],
            device_id={"pipe": stage + 1, "exp": along(k)},
            device_id_type=MESH,
        )

    def y_token(m, at, dz, dy):
        here = tokens.at[m, block(at)]
        return pltpu.make_async_remote_copy(
            src_ref=here,
            dst_ref=here,
            send_sem=f_sem.at[m, dz * max(1, ys - 1) + dy - 1],
            recv_sem=ar_sem.at[m, at],
            device_id={"pair": across(dy)},
            device_id_type=MESH,
        )

    def y_copy(m, dy, tz):
        return pltpu.make_async_remote_copy(
            src_ref=part.at[m, block(across(dy) * zs + tz)],
            dst_ref=fromy.at[m, dy - 1, tz],
            send_sem=y_sem.at[m, dy - 1, tz],
            recv_sem=yr_sem.at[m, dy - 1, tz],
            device_id={"pair": across(dy)},
            device_id_type=MESH,
        )

    def z_copy(m, k, source):
        return pltpu.make_async_remote_copy(
            src_ref=zsend.at[m, k],
            dst_ref=fromz.at[m, source],
            send_sem=z_sem.at[m, k - 1],
            recv_sem=zr_sem.at[m, source],
            device_id={"exp": along(k)},
            device_id_type=MESH,
        )

    def hand_copy(m):
        return pltpu.make_async_remote_copy(
            src_ref=obuf.at[m],
            dst_ref=hbuf.at[m],
            send_sem=hs_sem.at[m],
            recv_sem=h_sem.at[m],
            device_id={"pipe": stage + 1},
            device_id_type=MESH,
        )

    def out_copy(m):
        return pltpu.make_async_copy(obuf.at[m], out_ref.at[0, m], o_sem.at[m])

    def normed(state, gain):
        scale = lax.rsqrt(jnp.mean(state * state, axis=-1, keepdims=True) + EPS)
        return (state * scale * gain[...]).astype(BF16)

    def announce(m):
        from_input(m).wait()
        tokens[m, block(slot)] = normed(hbuf[m].astype(F32), gain_ref)
        for k in range(zs - 1, 0, -1):
            z_token(m, k).start()

    def relay_announce(m):
        relay_input(m).wait()
        relay[m, block(slot)] = normed(relay[m, block(slot)].astype(F32), gfirst)
        for k in range(zs - 1, 0, -1):
            relay_z(m, k).start()

    def relay_near(m):
        for dz in range(zs):
            at = y * zs + along(dz)
            if dz:
                relay_y(m, at, dz, 0).wait_recv()
            for dy in range(1, ys):
                relay_y(m, at, dz, dy).start()
            relay_x(m, at).start()

    def relay_far(m):
        for dy in range(1, ys):
            for dz in range(zs):
                at = across(dy) * zs + along(dz)
                relay_y(m, at, dz, dy).wait_recv()
                relay_x(m, at).start()

    def forward(m):
        for dz in range(zs):
            at = y * zs + along(dz)
            if dz:
                y_token(m, at, dz, 0).wait_recv()
            else:

                @pl.when(has_last)
                def _():
                    y_token(m, at, dz, 0).wait_recv()

            for dy in range(1, ys):
                y_token(m, at, dz, dy).start()

    def arrive(m):
        @pl.when(jnp.logical_and(is_first, m >= local))
        def _():
            for dz in range(zs):
                relay_x(m, y * zs + along(dz)).wait_recv()

        for dy in range(1, ys):
            for dz in range(zs):
                y_token(m, across(dy) * zs + along(dz), dz, dy).wait_recv()

    ftile = divisor_tile(ff, 256)
    ntile = divisor_tile(width, 512)
    count = groups * rows

    def spread():
        ids = lax.broadcasted_iota(jnp.int32, (groups, experts, span), 1)
        held = share[...]
        mine = [
            jnp.sum(jnp.where(ids == me * locals_ + j, held, 0.0), axis=1)
            for j in range(locals_)
        ]
        padding = jnp.zeros((128 - locals_ * groups, span), F32)
        column[...] = jnp.transpose(jnp.concatenate(mine + [padding], axis=0))

    def upper(m):
        weights = column[pl.ds(pl.multiple_of(m * rows, rows), rows)]
        for j in range(locals_):
            scaled = jnp.concatenate(
                [weights[:, j * groups + g : j * groups + g + 1] for g in range(groups)], axis=0
            )

            @pl.when(m == 0)
            def _():
                loads[j][0].wait()
                loads[j][1].wait()

            for c in range(0, ff, ftile):
                held = tokens[m]
                gate = jnp.dot(held, wg[j, :, c : c + ftile], preferred_element_type=F32)
                upward = jnp.dot(held, wu[j, :, c : c + ftile], preferred_element_type=F32)
                hid[:, j * ff + c : j * ff + c + ftile] = (
                    jax.nn.silu(gate) * upward * scaled
                ).astype(BF16)

    def lower(m):
        @pl.when(m == 0)
        def _():
            for j in range(locals_):
                loads[j][2].wait()

        for c in range(0, width, ntile):
            part[m, :, c : c + ntile] = jnp.dot(
                hid[...], wd[:, c : c + ntile], preferred_element_type=F32
            ).astype(BF16)

    def compute(m):
        arrive(m)
        upper(m)
        lower(m)
        for dy in range(1, ys):
            for k in range(zs - 1, -1, -1):
                y_copy(m, dy, along(k)).start()

    def own_part(m, pz):
        return part[m, block(y * zs + pz)].astype(F32)

    def scatter(m):
        for k in range(zs - 1, 0, -1):
            pz = along(k)
            total = own_part(m, pz)
            for dy in range(1, ys):
                y_copy(m, dy, pz).wait_recv()
                total = total + fromy[m, dy - 1, pz].astype(F32)
            zsend[m, k] = total.astype(BF16)
            z_copy(m, k, z).start()

    def finish(m):
        @pl.when(jnp.logical_or(has_last, m >= local))
        def _():
            from_input(m).wait()

        total = hbuf[m].astype(F32) + own_part(m, z)
        for dy in range(1, ys):
            y_copy(m, dy, z).wait_recv()
            total = total + fromy[m, dy - 1, z].astype(F32)
        for k in range(1, zs):
            z_copy(m, k, along(k)).wait_recv()
            total = total + fromz[m, along(k)].astype(F32)
        state = total.astype(BF16)
        obuf[m] = state

        @pl.when(has_next)
        def _():
            nbuf[m] = normed(state.astype(F32), gnext)
            for k in range(zs - 1, -1, -1):
                next_token(m, k).start()
            hand_copy(m).start()

        out_copy(m).start()

    @pl.when(is_first)
    def _():
        if local < micro:
            first_gain_copy().start()
        for m in range(local):
            announce(m)

    @pl.when(has_last)
    def _():
        gain_copy().start()

    share_send()

    @pl.when(is_helper)
    def _():
        if local < micro:
            first_gain_copy().wait_recv()
            for m in range(local, min(micro, local + RELAY_AHEAD)):
                relay_announce(m)

            @pl.loop(local, micro + 1)
            def _(m):
                @pl.when(m < micro)
                def _():
                    relay_near(m)

                @pl.when(m + RELAY_AHEAD < micro)
                def _():
                    relay_announce(m + RELAY_AHEAD)

                @pl.when(m > local)
                def _():
                    relay_far(m - 1)

    @pl.when(has_next)
    def _():
        gain_copy().wait_recv()

    share_wait()
    spread()
    handlers = {"F": forward, "S": scatter, "E": finish}
    plans = plan_of(stages, micro, local)

    @pl.loop(0, micro + 1)
    def _(step):
        for at, plan in enumerate(plans):

            @pl.when(stage == at)
            def _():
                for name, table in plan:
                    m = jnp.int32(-1)
                    for when, piece in table:
                        m = jnp.where(step == when, piece, m)

                    @pl.when(m >= 0)
                    def _():
                        handlers[name](m)

        @pl.when(step < micro)
        def _():
            compute(step)

    for dz, dy in others:
        pz, py = peer(dz, dy)
        share_copy(slot, pz, py).wait_send()

    @pl.when(has_last)
    def _():
        gain_copy().wait_send()

    if local < micro:

        @pl.when(is_first)
        def _():
            first_gain_copy().wait_send()

        @pl.when(is_helper)
        def _():
            @pl.loop(local, micro)
            def _(m):
                for k in range(1, zs):
                    relay_z(m, k).wait_send()
                for dz in range(zs):
                    for dy in range(1, ys):
                        relay_y(m, slot, dz, dy).wait_send()
                for at in range(groups):
                    relay_x(m, at).wait_send()

    @pl.loop(0, micro)
    def _(m):
        for k in range(1, zs):
            z_copy(m, k, z).wait_send()

        direct = jnp.logical_or(has_last, m < local)

        @pl.when(jnp.logical_and(is_first, direct))
        def _():
            for k in range(1, zs):
                z_token(m, k).wait_send()

        @pl.when(direct)
        def _():
            for dy in range(1, ys):
                for tz in range(zs):
                    y_token(m, slot, tz, dy).wait_send()

        @pl.when(has_next)
        def _():
            for k in range(zs):
                next_token(m, k).wait_send()
            hand_copy(m).wait_send()

        for dy in range(1, ys):
            for tz in range(zs):
                y_copy(m, dy, tz).wait_send()

        out_copy(m).wait()


def relayed(hidden_in, routes, gate_probs, norm_gain, w_gate, w_up, w_down):
    batches, whole_rows, _ = hidden_in.shape
    pieces = PIECES if whole_rows % (16 * PIECES) == 0 else 1
    hidden_in = cut(hidden_in, 0, pieces)
    routes = jnp.transpose(routes, (0, 1, 3, 2))
    gate_probs = jnp.transpose(gate_probs, (0, 1, 3, 2))
    micro, rows, width = hidden_in.shape
    _, locals_, _, ff = w_gate.shape
    stages, zs, ys = (lax.axis_size(a) for a in ("pipe", "exp", "pair"))
    groups = zs * ys
    dma = pltpu.SemaphoreType.DMA
    anywhere = pl.BlockSpec(memory_space=pl.ANY)
    inside = pl.BlockSpec(memory_space=pltpu.VMEM)
    out = pl.pallas_call(
        functools.partial(relay_kernel, stages, zs, ys),
        out_shape=jax.ShapeDtypeStruct((1, micro, rows, width), BF16),
        in_specs=[anywhere, inside, inside, inside, anywhere, anywhere, anywhere],
        out_specs=anywhere,
        scratch_shapes=[
            pltpu.VMEM((locals_, width, ff), BF16),
            pltpu.VMEM((locals_, width, ff), BF16),
            pltpu.VMEM((locals_ * ff, width), BF16),
            pltpu.VMEM((micro, rows, width), BF16),
            pltpu.VMEM((micro, groups * rows, width), BF16),
            pltpu.VMEM((groups, groups * locals_, micro * rows), F32),
            pltpu.VMEM((micro * rows, 128), F32),
            pltpu.VMEM((groups * rows, locals_ * ff), BF16),
            pltpu.VMEM((micro, groups * rows, width), BF16),
            pltpu.VMEM((micro, max(1, ys - 1), zs, rows, width), BF16),
            pltpu.VMEM((micro, zs, rows, width), BF16),
            pltpu.VMEM((micro, zs, rows, width), BF16),
            pltpu.VMEM((micro, rows, width), BF16),
            pltpu.VMEM((micro, rows, width), BF16),
            pltpu.VMEM((1, width), F32),
            pltpu.VMEM((micro, groups * rows, width), BF16),
            pltpu.VMEM((1, width), F32),
            dma((3 * locals_,)),
            dma((micro,)),
            dma((micro,)),
            dma((micro,)),
            dma((groups,)),
            dma((groups,)),
            dma((micro, zs)),
            dma((micro, groups)),
            dma((micro, zs * max(1, ys - 1))),
            dma((micro, max(1, ys - 1), zs)),
            dma((micro, max(1, ys - 1), zs)),
            dma((micro, max(1, zs - 1))),
            dma((micro, zs)),
            dma((2,)),
            dma((2,)),
            dma((micro,)),
            dma((micro, zs)),
            dma((micro, groups)),
            dma((micro, zs * max(1, ys - 1))),
            dma((micro, groups)),
        ],
        compiler_params=pltpu.CompilerParams(
            collective_id=0, has_side_effects=True, vmem_limit_bytes=VMEM_LIMIT
        ),
    )(hidden_in, routes, gate_probs, norm_gain, w_gate, w_up, w_down)
    return out.reshape(1, batches, whole_rows, width)


def cut(value, axis, pieces):
    shape = value.shape
    rows = shape[axis + 1] // pieces
    return value.reshape(shape[:axis] + (shape[axis] * pieces, rows) + shape[axis + 2 :])


def kernel_fits(hidden_in, w_gate, groups):
    micro, rows, width = hidden_in.shape
    _, locals_, _, ff = w_gate.shape
    weights = 3 * locals_ * width * ff
    moved = micro * rows * width * (5 * groups + 6)
    small = groups * rows * (locals_ * ff + 2 * micro * groups * locals_)
    fits = 2 * (weights + moved + small) + 8 * 1024 * 1024 < VMEM_LIMIT
    small_enough = groups * locals_ <= 128 and micro * rows % 128 == 0
    return fits and small_enough and rows % 16 == 0 and width % 128 == 0 and ff % 128 == 0


def passed_along(value, axis, steps):
    count = lax.axis_size(axis)
    first, last = (max(0, -steps), min(count, count - steps))
    return lax.ppermute(value, axis, [(source, source + steps) for source in range(first, last)])


def expert_block(arrived, wgate, wupper, wdown):
    gate = jnp.einsum("nlcd,ldf->nlcf", arrived, wgate, preferred_element_type=jnp.float32)
    upward = jnp.einsum("nlcd,ldf->nlcf", arrived, wupper, preferred_element_type=jnp.float32)
    hidden = (jax.nn.silu(gate) * upward).astype(jnp.bfloat16)
    return jnp.einsum("nlcf,lfd->nlcd", hidden, wdown, preferred_element_type=jnp.float32).astype(
        jnp.bfloat16
    )


def on_device(hidden_in, routes, gate_probs, norm_gain, w_gate, w_up, w_down):
    if kernel_fits(hidden_in, w_gate, lax.axis_size(("exp", "pair"))):
        return relayed(hidden_in, routes, gate_probs, norm_gain, w_gate, w_up, w_down)
    section = lax.axis_index("pipe")
    micro, tok_rows, width = hidden_in.shape
    top_count = routes.shape[3]
    groups = lax.axis_size(("exp", "pair"))
    local_experts = w_gate.shape[1]
    experts = local_experts * groups
    capacity = max(2, 3 * tok_rows * top_count // (2 * experts))
    gain = norm_gain[0]
    wgate = w_gate[0]
    wupper = w_up[0]
    wdown = w_down[0]
    expert_ids = jnp.arange(experts, dtype=jnp.int32)

    def layer(state, index):
        chosen = lax.dynamic_index_in_dim(routes[0], index, 0, keepdims=False).reshape(-1)
        probs = lax.dynamic_index_in_dim(gate_probs[0], index, 0, keepdims=False)
        floated = state.astype(jnp.float32)
        scale = lax.rsqrt(jnp.mean(floated * floated, axis=-1, keepdims=True) + EPS)
        normed = (floated * scale * gain).astype(jnp.bfloat16)
        onehot = (chosen[:, None] == expert_ids[None, :]).astype(jnp.int32)
        before = jnp.cumsum(onehot, axis=0) - onehot
        slots = jnp.sum(before * onehot, axis=1)
        outgoing = jnp.zeros((experts, capacity, width), jnp.bfloat16)
        outgoing = outgoing.at[chosen, slots].set(jnp.repeat(normed, top_count, axis=0))
        grouped = outgoing.reshape(groups, local_experts, capacity, width)
        produced = expert_block(
            lax.all_to_all(grouped, ("exp", "pair"), split_axis=0, concat_axis=0, tiled=True),
            wgate,
            wupper,
            wdown,
        )
        returned = lax.all_to_all(
            produced, ("exp", "pair"), split_axis=0, concat_axis=0, tiled=True
        )
        results = returned.reshape(experts, capacity, width)[chosen, slots]
        results = results.reshape(tok_rows, top_count, width).astype(jnp.float32)
        weights = probs / jnp.sum(probs, axis=-1, keepdims=True)
        mixed = jnp.einsum("tk,tkd->td", weights, results)
        return (floated + mixed).astype(jnp.bfloat16)

    def advance(step, carry):
        received, saved = carry
        index = step - section
        valid = jnp.logical_and(index >= 0, index < micro)
        clipped = jnp.clip(index, 0, micro - 1)
        first = lax.dynamic_index_in_dim(hidden_in, clipped, 0, keepdims=False)
        state = jnp.where(section == 0, first, received)
        updated = layer(state, clipped)
        saved = jnp.where(valid, lax.dynamic_update_index_in_dim(saved, updated, clipped, 0), saved)
        received = passed_along(updated, "pipe", 1)
        return (received, saved)

    start = (
        jnp.zeros((tok_rows, width), jnp.bfloat16),
        jnp.zeros((micro, tok_rows, width), jnp.bfloat16),
    )
    received, saved = lax.fori_loop(0, micro + lax.axis_size("pipe") - 1, advance, start)
    return saved[None]


def solution(mesh):
    in_specs = (
        P(None, ("exp", "pair"), None),
        P("pipe", None, ("exp", "pair"), None),
        P("pipe", None, ("exp", "pair"), None),
        P("pipe", None),
        P("pipe", ("exp", "pair"), None, None),
        P("pipe", ("exp", "pair"), None, None),
        P("pipe", ("exp", "pair"), None, None),
    )
    out_specs = P("pipe", None, ("exp", "pair"), None)
    return jax.shard_map(
        on_device, mesh=mesh, in_specs=in_specs, out_specs=out_specs, check_vma=False
    )
```

```python
import functools

import jax
import jax.numpy as jnp
from jax import lax
from jax.experimental import pallas as pl
from jax.experimental.pallas import tpu as pltpu
from jax.sharding import PartitionSpec as P

EPS = 1e-06
MESH = pl.DeviceIdType.MESH
F32 = jnp.float32
BF16 = jnp.bfloat16
PIECES = 2
RELAY_AHEAD = 2
LOCAL = 2
SCHEDULE = (
    ("FF", "", "S", "SE", "SE", "SE", "SE", "SE", "SESEE"),
    ("FF", "", "SFEFS", "ES", "EFS", "ESFEF", "S", "EFSE", "SE"),
    ("F", "FS", "ESFFE", "", "FSSFE", "", "FSEEF", "S", "SESEE"),
    ("F", "SF", "SF", "FESFE", "FE", "F", "SFS", "SEE", "SSEEE"),
)
VMEM_LIMIT = 63 * 1024 * 1024


def divisor_tile(size, most):
    tile = most
    while size % tile:
        tile //= 2
    return tile


def merged(one, two):
    best = {(len(one), len(two)): ""}
    for i in range(len(one), -1, -1):
        for j in range(len(two), -1, -1):
            options = []
            if i < len(one) and j < len(two) and one[i] == two[j]:
                options.append(one[i] + best[i + 1, j + 1])
            if i < len(one):
                options.append(one[i] + best[i + 1, j])
            if j < len(two):
                options.append(two[j] + best[i, j + 1])
            if options:
                best[i, j] = min(options, key=len)
    return best[0, 0]


def plan_of(stages, micro, local):
    tuned = len(SCHEDULE) == stages and len(SCHEDULE[0]) == micro + 1 and local == LOCAL
    plans = []
    for at in range(stages):
        if tuned:
            gaps = SCHEDULE[at]
        elif at == 0:
            gaps = ("F" * local,) + ("SE",) * micro
        else:
            gaps = ("F",) + ("SFE",) * (micro - 1) + ("SE",)
        slots = functools.reduce(merged, gaps)
        tables = [[] for _ in slots]
        counts = {}
        for step, gap in enumerate(gaps):
            place = 0
            for name in gap:
                place = slots.index(name, place)
                tables[place].append((step, counts.get(name, 0)))
                counts[name] = counts.get(name, 0) + 1
                place += 1
        plans.append(list(zip(slots, tables)))
    return plans


def relay_kernel(
    stages,
    zs,
    ys,
    hidden_ref,
    routes_ref,
    probs_ref,
    gain_ref,
    wgate_ref,
    wup_ref,
    wdown_ref,
    out_ref,
    wg,
    wu,
    wd,
    hbuf,
    tokens,
    share,
    column,
    hid,
    part,
    fromy,
    zsend,
    fromz,
    obuf,
    nbuf,
    gnext,
    relay,
    gfirst,
    w_sem,
    h_sem,
    hs_sem,
    o_sem,
    s_sem,
    sr_sem,
    a_sem,
    ar_sem,
    f_sem,
    y_sem,
    yr_sem,
    z_sem,
    zr_sem,
    g_sem,
    gr_sem,
    hr_sem,
    b_sem,
    rr_sem,
    q_sem,
    v_sem,
):
    micro, rows, width = hbuf.shape
    locals_, _, ff = wg.shape
    span = share.shape[2]
    groups = zs * ys
    experts = groups * locals_
    stage = lax.axis_index("pipe")
    z = lax.axis_index("exp")
    y = lax.axis_index("pair")
    me = z * ys + y
    slot = y * zs + z
    upper_half = lax.div(2 * z, zs)
    turn = 1 - 2 * upper_half
    is_first = stage == 0
    has_last = stage > 0
    has_next = stage < stages - 1
    helper = stages // 2
    local = min(LOCAL, micro) if helper else micro
    is_helper = jnp.logical_and(stage == helper, stage > 0)

    def block(at):
        return pl.ds(pl.multiple_of(at * rows, rows), rows)

    def along(k):
        return lax.rem(z + turn * k + zs, zs)

    def across(dy):
        return lax.rem(y + dy, ys)

    def peer(dz, dy):
        return lax.rem(z + dz, zs), lax.rem(y + dy, ys)

    others = [(dz, dy) for dy in range(ys) for dz in range(zs) if dz or dy]

    loads = []
    for j in range(locals_):
        loads.append(
            (
                pltpu.make_async_copy(wgate_ref.at[0, j], wg.at[j], w_sem.at[3 * j]),
                pltpu.make_async_copy(wup_ref.at[0, j], wu.at[j], w_sem.at[3 * j + 1]),
                pltpu.make_async_copy(
                    wdown_ref.at[0, j], wd.at[pl.ds(j * ff, ff)], w_sem.at[3 * j + 2]
                ),
            )
        )

    def from_input(m):
        return pltpu.make_async_copy(hidden_ref.at[m], hbuf.at[m], h_sem.at[m])

    @pl.when(is_first)
    def _():
        for m in range(micro):
            from_input(m).start()

    def relay_input(m):
        here = relay.at[m, block(slot)]
        return pltpu.make_async_copy(hidden_ref.at[m], here, hr_sem.at[m])

    @pl.when(is_helper)
    def _():
        for m in range(local, micro):
            relay_input(m).start()

    for j in range(locals_):
        loads[j][0].start()
        loads[j][1].start()
    for j in range(locals_):
        loads[j][2].start()

    barrier = pltpu.get_barrier_semaphore()
    for dz, dy in others:
        pz, py = peer(dz, dy)
        pl.semaphore_signal(barrier, inc=1, device_id={"exp": pz, "pair": py}, device_id_type=MESH)

    @pl.when(has_last)
    def _():
        for k in range(zs):
            pl.semaphore_signal(
                barrier,
                inc=1,
                device_id={"pipe": stage - 1, "exp": along(k)},
                device_id_type=MESH,
            )

    @pl.when(has_next)
    def _():
        for k in range(zs):
            pl.semaphore_signal(
                barrier,
                inc=1,
                device_id={"pipe": stage + 1, "exp": along(k)},
                device_id_type=MESH,
            )

    if local < micro:

        @pl.when(is_first)
        def _():
            pl.semaphore_signal(
                barrier, inc=1, device_id={"pipe": helper}, device_id_type=MESH
            )

        @pl.when(is_helper)
        def _():
            pl.semaphore_signal(barrier, inc=1, device_id={"pipe": 0}, device_id_type=MESH)

    batches, top, held_rows = routes_ref.shape[1:]
    named_ids = lax.broadcasted_iota(jnp.int32, (experts, held_rows), 0)
    for m in range(batches):
        probs = probs_ref[0, m]
        normal = probs / jnp.sum(probs, axis=0, keepdims=True)
        chosen = routes_ref[0, m]
        total = jnp.zeros((experts, held_rows), F32)
        for k in range(top):
            total = total + jnp.where(
                named_ids == chosen[k : k + 1], normal[k : k + 1], 0.0
            )
        share[slot, :, m * held_rows : (m + 1) * held_rows] = total

    linked = has_last.astype(jnp.int32) + has_next.astype(jnp.int32)
    awaited = len(others) + linked * zs
    if local < micro:
        awaited = awaited + is_first.astype(jnp.int32) + is_helper.astype(jnp.int32)
    pl.semaphore_wait(barrier, awaited)

    def share_copy(at, to_z, to_y):
        return pltpu.make_async_remote_copy(
            src_ref=share.at[at],
            dst_ref=share.at[at],
            send_sem=s_sem.at[to_y * zs + to_z],
            recv_sem=sr_sem.at[at],
            device_id={"exp": to_z, "pair": to_y},
            device_id_type=MESH,
        )

    def share_send():
        for dz, dy in others:
            pz, py = peer(dz, dy)
            share_copy(slot, pz, py).start()

    def share_wait():
        for dz, dy in others:
            pz, py = peer(dz, dy)
            share_copy(py * zs + pz, pz, py).wait_recv()

    def gain_copy():
        return pltpu.make_async_remote_copy(
            src_ref=gain_ref,
            dst_ref=gnext,
            send_sem=g_sem.at[0],
            recv_sem=gr_sem.at[0],
            device_id={"pipe": stage - 1},
            device_id_type=MESH,
        )

    def first_gain_copy():
        return pltpu.make_async_remote_copy(
            src_ref=gain_ref,
            dst_ref=gfirst,
            send_sem=g_sem.at[1],
            recv_sem=gr_sem.at[1],
            device_id={"pipe": helper},
            device_id_type=MESH,
        )

    def relay_z(m, k):
        here = relay.at[m, block(slot)]
        return pltpu.make_async_remote_copy(
            src_ref=here,
            dst_ref=here,
            send_sem=b_sem.at[m, k],
            recv_sem=rr_sem.at[m, slot],
            device_id={"exp": along(k)},
            device_id_type=MESH,
        )

    def relay_y(m, at, dz, dy):
        here = relay.at[m, block(at)]
        return pltpu.make_async_remote_copy(
            src_ref=here,
            dst_ref=here,
            send_sem=q_sem.at[m, dz * max(1, ys - 1) + dy - 1],
            recv_sem=rr_sem.at[m, at],
            device_id={"pair": across(dy)},
            device_id_type=MESH,
        )

    def relay_x(m, at):
        return pltpu.make_async_remote_copy(
            src_ref=relay.at[m, block(at)],
            dst_ref=tokens.at[m, block(at)],
            send_sem=v_sem.at[m, at],
            recv_sem=ar_sem.at[m, at],
            device_id={"pipe": 0},
            device_id_type=MESH,
        )

    def z_token(m, k):
        here = tokens.at[m, block(slot)]
        return pltpu.make_async_remote_copy(
            src_ref=here,
            dst_ref=here,
            send_sem=a_sem.at[m, k],
            recv_sem=ar_sem.at[m, slot],
            device_id={"exp": along(k)},
            device_id_type=MESH,
        )

    def next_token(m, k):
        return pltpu.make_async_remote_copy(
            src_ref=nbuf.at[m],
            dst_ref=tokens.at[m, block(slot)],
            send_sem=a_sem.at[m, k],
            recv_sem=ar_sem.at[m, slot],
            device_id={"pipe": stage + 1, "exp": along(k)},
            device_id_type=MESH,
        )

    def y_token(m, at, dz, dy):
        here = tokens.at[m, block(at)]
        return pltpu.make_async_remote_copy(
            src_ref=here,
            dst_ref=here,
            send_sem=f_sem.at[m, dz * max(1, ys - 1) + dy - 1],
            recv_sem=ar_sem.at[m, at],
            device_id={"pair": across(dy)},
            device_id_type=MESH,
        )

    def y_copy(m, dy, tz):
        return pltpu.make_async_remote_copy(
            src_ref=part.at[m, block(across(dy) * zs + tz)],
            dst_ref=fromy.at[m, dy - 1, tz],
            send_sem=y_sem.at[m, dy - 1, tz],
            recv_sem=yr_sem.at[m, dy - 1, tz],
            device_id={"pair": across(dy)},
            device_id_type=MESH,
        )

    def z_copy(m, k, source):
        return pltpu.make_async_remote_copy(
            src_ref=zsend.at[m, k],
            dst_ref=fromz.at[m, source],
            send_sem=z_sem.at[m, k - 1],
            recv_sem=zr_sem.at[m, source],
            device_id={"exp": along(k)},
            device_id_type=MESH,
        )

    def hand_copy(m):
        return pltpu.make_async_remote_copy(
            src_ref=obuf.at[m],
            dst_ref=hbuf.at[m],
            send_sem=hs_sem.at[m],
            recv_sem=h_sem.at[m],
            device_id={"pipe": stage + 1},
            device_id_type=MESH,
        )

    def out_copy(m):
        return pltpu.make_async_copy(obuf.at[m], out_ref.at[0, m], o_sem.at[m])

    def normed(state, gain):
        scale = lax.rsqrt(jnp.mean(state * state, axis=-1, keepdims=True) + EPS)
        return (state * scale * gain[...]).astype(BF16)

    def announce(m):
        from_input(m).wait()
        tokens[m, block(slot)] = normed(hbuf[m].astype(F32), gain_ref)
        for k in range(zs - 1, 0, -1):
            z_token(m, k).start()

    def relay_announce(m):
        relay_input(m).wait()
        relay[m, block(slot)] = normed(relay[m, block(slot)].astype(F32), gfirst)
        for k in range(zs - 1, 0, -1):
            relay_z(m, k).start()

    def relay_near(m):
        for dz in range(zs):
            at = y * zs + along(dz)
            if dz:
                relay_y(m, at, dz, 0).wait_recv()
            for dy in range(1, ys):
                relay_y(m, at, dz, dy).start()
            relay_x(m, at).start()

    def relay_far(m):
        for dy in range(1, ys):
            for dz in range(zs):
                at = across(dy) * zs + along(dz)
                relay_y(m, at, dz, dy).wait_recv()
                relay_x(m, at).start()

    def forward(m):
        for dz in range(zs):
            at = y * zs + along(dz)
            if dz:
                y_token(m, at, dz, 0).wait_recv()
            else:

                @pl.when(has_last)
                def _():
                    y_token(m, at, dz, 0).wait_recv()

            for dy in range(1, ys):
                y_token(m, at, dz, dy).start()

    def arrive(m):
        @pl.when(jnp.logical_and(is_first, m >= local))
        def _():
            for dz in range(zs):
                relay_x(m, y * zs + along(dz)).wait_recv()

        for dy in range(1, ys):
            for dz in range(zs):
                y_token(m, across(dy) * zs + along(dz), dz, dy).wait_recv()

    ftile = divisor_tile(ff, 256)
    ntile = divisor_tile(width, 512)
    count = groups * rows

    def spread():
        ids = lax.broadcasted_iota(jnp.int32, (groups, experts, span), 1)
        held = share[...]
        mine = [
            jnp.sum(jnp.where(ids == me * locals_ + j, held, 0.0), axis=1)
            for j in range(locals_)
        ]
        padding = jnp.zeros((128 - locals_ * groups, span), F32)
        column[...] = jnp.transpose(jnp.concatenate(mine + [padding], axis=0))

    def upper(m):
        weights = column[pl.ds(pl.multiple_of(m * rows, rows), rows)]
        for j in range(locals_):
            scaled = jnp.concatenate(
                [weights[:, j * groups + g : j * groups + g + 1] for g in range(groups)], axis=0
            )

            @pl.when(m == 0)
            def _():
                loads[j][0].wait()
                loads[j][1].wait()

            for c in range(0, ff, ftile):
                held = tokens[m]
                gate = jnp.dot(held, wg[j, :, c : c + ftile], preferred_element_type=F32)
                upward = jnp.dot(held, wu[j, :, c : c + ftile], preferred_element_type=F32)
                hid[:, j * ff + c : j * ff + c + ftile] = (
                    jax.nn.silu(gate) * upward * scaled
                ).astype(BF16)

    def lower(m):
        @pl.when(m == 0)
        def _():
            for j in range(locals_):
                loads[j][2].wait()

        for c in range(0, width, ntile):
            part[m, :, c : c + ntile] = jnp.dot(
                hid[...], wd[:, c : c + ntile], preferred_element_type=F32
            ).astype(BF16)

    def compute(m):
        arrive(m)
        upper(m)
        lower(m)
        for dy in range(1, ys):
            for k in range(zs - 1, -1, -1):
                y_copy(m, dy, along(k)).start()

    def own_part(m, pz):
        return part[m, block(y * zs + pz)].astype(F32)

    def scatter(m):
        for k in range(zs - 1, 0, -1):
            pz = along(k)
            total = own_part(m, pz)
            for dy in range(1, ys):
                y_copy(m, dy, pz).wait_recv()
                total = total + fromy[m, dy - 1, pz].astype(F32)
            zsend[m, k] = total.astype(BF16)
            z_copy(m, k, z).start()

    def finish(m):
        @pl.when(jnp.logical_or(has_last, m >= local))
        def _():
            from_input(m).wait()

        total = hbuf[m].astype(F32) + own_part(m, z)
        for dy in range(1, ys):
            y_copy(m, dy, z).wait_recv()
            total = total + fromy[m, dy - 1, z].astype(F32)
        for k in range(1, zs):
            z_copy(m, k, along(k)).wait_recv()
            total = total + fromz[m, along(k)].astype(F32)
        state = total.astype(BF16)
        obuf[m] = state

        @pl.when(has_next)
        def _():
            nbuf[m] = normed(state.astype(F32), gnext)
            for k in range(zs - 1, -1, -1):
                next_token(m, k).start()
            hand_copy(m).start()

        out_copy(m).start()

    @pl.when(is_first)
    def _():
        if local < micro:
            first_gain_copy().start()
        for m in range(local):
            announce(m)

    @pl.when(has_last)
    def _():
        gain_copy().start()

    share_send()

    @pl.when(is_helper)
    def _():
        if local < micro:
            first_gain_copy().wait_recv()
            for m in range(local, min(micro, local + RELAY_AHEAD)):
                relay_announce(m)

            @pl.loop(local, micro + 1)
            def _(m):
                @pl.when(m < micro)
                def _():
                    relay_near(m)

                @pl.when(m + RELAY_AHEAD < micro)
                def _():
                    relay_announce(m + RELAY_AHEAD)

                @pl.when(m > local)
                def _():
                    relay_far(m - 1)

    @pl.when(has_next)
    def _():
        gain_copy().wait_recv()

    share_wait()
    spread()
    handlers = {"F": forward, "S": scatter, "E": finish}
    plans = plan_of(stages, micro, local)

    @pl.loop(0, micro + 1)
    def _(step):
        for at, plan in enumerate(plans):

            @pl.when(stage == at)
            def _():
                for name, table in plan:
                    m = jnp.int32(-1)
                    for when, piece in table:
                        m = jnp.where(step == when, piece, m)

                    @pl.when(m >= 0)
                    def _():
                        handlers[name](m)

        @pl.when(step < micro)
        def _():
            compute(step)

    for dz, dy in others:
        pz, py = peer(dz, dy)
        share_copy(slot, pz, py).wait_send()

    @pl.when(has_last)
    def _():
        gain_copy().wait_send()

    if local < micro:

        @pl.when(is_first)
        def _():
            first_gain_copy().wait_send()

        @pl.when(is_helper)
        def _():
            @pl.loop(local, micro)
            def _(m):
                for k in range(1, zs):
                    relay_z(m, k).wait_send()
                for dz in range(zs):
                    for dy in range(1, ys):
                        relay_y(m, slot, dz, dy).wait_send()
                for at in range(groups):
                    relay_x(m, at).wait_send()

    @pl.loop(0, micro)
    def _(m):
        for k in range(1, zs):
            z_copy(m, k, z).wait_send()

        direct = jnp.logical_or(has_last, m < local)

        @pl.when(jnp.logical_and(is_first, direct))
        def _():
            for k in range(1, zs):
                z_token(m, k).wait_send()

        @pl.when(direct)
        def _():
            for dy in range(1, ys):
                for tz in range(zs):
                    y_token(m, slot, tz, dy).wait_send()

        @pl.when(has_next)
        def _():
            for k in range(zs):
                next_token(m, k).wait_send()
            hand_copy(m).wait_send()

        for dy in range(1, ys):
            for tz in range(zs):
                y_copy(m, dy, tz).wait_send()

        out_copy(m).wait()


def relayed(hidden_in, routes, gate_probs, norm_gain, w_gate, w_up, w_down):
    batches, whole_rows, _ = hidden_in.shape
    pieces = PIECES if whole_rows % (16 * PIECES) == 0 else 1
    hidden_in = cut(hidden_in, 0, pieces)
    routes = jnp.transpose(routes, (0, 1, 3, 2))
    gate_probs = jnp.transpose(gate_probs, (0, 1, 3, 2))
    micro, rows, width = hidden_in.shape
    _, locals_, _, ff = w_gate.shape
    stages, zs, ys = (lax.axis_size(a) for a in ("pipe", "exp", "pair"))
    groups = zs * ys
    dma = pltpu.SemaphoreType.DMA
    anywhere = pl.BlockSpec(memory_space=pl.ANY)
    inside = pl.BlockSpec(memory_space=pltpu.VMEM)
    out = pl.pallas_call(
        functools.partial(relay_kernel, stages, zs, ys),
        out_shape=jax.ShapeDtypeStruct((1, micro, rows, width), BF16),
        in_specs=[anywhere, inside, inside, inside, anywhere, anywhere, anywhere],
        out_specs=anywhere,
        scratch_shapes=[
            pltpu.VMEM((locals_, width, ff), BF16),
            pltpu.VMEM((locals_, width, ff), BF16),
            pltpu.VMEM((locals_ * ff, width), BF16),
            pltpu.VMEM((micro, rows, width), BF16),
            pltpu.VMEM((micro, groups * rows, width), BF16),
            pltpu.VMEM((groups, groups * locals_, micro * rows), F32),
            pltpu.VMEM((micro * rows, 128), F32),
            pltpu.VMEM((groups * rows, locals_ * ff), BF16),
            pltpu.VMEM((micro, groups * rows, width), BF16),
            pltpu.VMEM((micro, max(1, ys - 1), zs, rows, width), BF16),
            pltpu.VMEM((micro, zs, rows, width), BF16),
            pltpu.VMEM((micro, zs, rows, width), BF16),
            pltpu.VMEM((micro, rows, width), BF16),
            pltpu.VMEM((micro, rows, width), BF16),
            pltpu.VMEM((1, width), F32),
            pltpu.VMEM((micro, groups * rows, width), BF16),
            pltpu.VMEM((1, width), F32),
            dma((3 * locals_,)),
            dma((micro,)),
            dma((micro,)),
            dma((micro,)),
            dma((groups,)),
            dma((groups,)),
            dma((micro, zs)),
            dma((micro, groups)),
            dma((micro, zs * max(1, ys - 1))),
            dma((micro, max(1, ys - 1), zs)),
            dma((micro, max(1, ys - 1), zs)),
            dma((micro, max(1, zs - 1))),
            dma((micro, zs)),
            dma((2,)),
            dma((2,)),
            dma((micro,)),
            dma((micro, zs)),
            dma((micro, groups)),
            dma((micro, zs * max(1, ys - 1))),
            dma((micro, groups)),
        ],
        compiler_params=pltpu.CompilerParams(
            collective_id=0, has_side_effects=True, vmem_limit_bytes=VMEM_LIMIT
        ),
    )(hidden_in, routes, gate_probs, norm_gain, w_gate, w_up, w_down)
    return out.reshape(1, batches, whole_rows, width)


def cut(value, axis, pieces):
    shape = value.shape
    rows = shape[axis + 1] // pieces
    return value.reshape(shape[:axis] + (shape[axis] * pieces, rows) + shape[axis + 2 :])


def kernel_fits(hidden_in, w_gate, groups):
    micro, rows, width = hidden_in.shape
    _, locals_, _, ff = w_gate.shape
    weights = 3 * locals_ * width * ff
    moved = micro * rows * width * (5 * groups + 6)
    small = groups * rows * (locals_ * ff + 2 * micro * groups * locals_)
    fits = 2 * (weights + moved + small) + 8 * 1024 * 1024 < VMEM_LIMIT
    small_enough = groups * locals_ <= 128 and micro * rows % 128 == 0
    return fits and small_enough and rows % 16 == 0 and width % 128 == 0 and ff % 128 == 0


def passed_along(value, axis, steps):
    count = lax.axis_size(axis)
    first, last = (max(0, -steps), min(count, count - steps))
    return lax.ppermute(value, axis, [(source, source + steps) for source in range(first, last)])


def expert_block(arrived, wgate, wupper, wdown):
    gate = jnp.einsum("nlcd,ldf->nlcf", arrived, wgate, preferred_element_type=jnp.float32)
    upward = jnp.einsum("nlcd,ldf->nlcf", arrived, wupper, preferred_element_type=jnp.float32)
    hidden = (jax.nn.silu(gate) * upward).astype(jnp.bfloat16)
    return jnp.einsum("nlcf,lfd->nlcd", hidden, wdown, preferred_element_type=jnp.float32).astype(
        jnp.bfloat16
    )


def on_device(hidden_in, routes, gate_probs, norm_gain, w_gate, w_up, w_down):
    if kernel_fits(hidden_in, w_gate, lax.axis_size(("exp", "pair"))):
        return relayed(hidden_in, routes, gate_probs, norm_gain, w_gate, w_up, w_down)
    section = lax.axis_index("pipe")
    micro, tok_rows, width = hidden_in.shape
    top_count = routes.shape[3]
    groups = lax.axis_size(("exp", "pair"))
    local_experts = w_gate.shape[1]
    experts = local_experts * groups
    capacity = max(2, 3 * tok_rows * top_count // (2 * experts))
    gain = norm_gain[0]
    wgate = w_gate[0]
    wupper = w_up[0]
    wdown = w_down[0]
    expert_ids = jnp.arange(experts, dtype=jnp.int32)

    def layer(state, index):
        chosen = lax.dynamic_index_in_dim(routes[0], index, 0, keepdims=False).reshape(-1)
        probs = lax.dynamic_index_in_dim(gate_probs[0], index, 0, keepdims=False)
        floated = state.astype(jnp.float32)
        scale = lax.rsqrt(jnp.mean(floated * floated, axis=-1, keepdims=True) + EPS)
        normed = (floated * scale * gain).astype(jnp.bfloat16)
        onehot = (chosen[:, None] == expert_ids[None, :]).astype(jnp.int32)
        before = jnp.cumsum(onehot, axis=0) - onehot
        slots = jnp.sum(before * onehot, axis=1)
        outgoing = jnp.zeros((experts, capacity, width), jnp.bfloat16)
        outgoing = outgoing.at[chosen, slots].set(jnp.repeat(normed, top_count, axis=0))
        grouped = outgoing.reshape(groups, local_experts, capacity, width)
        produced = expert_block(
            lax.all_to_all(grouped, ("exp", "pair"), split_axis=0, concat_axis=0, tiled=True),
            wgate,
            wupper,
            wdown,
        )
        returned = lax.all_to_all(
            produced, ("exp", "pair"), split_axis=0, concat_axis=0, tiled=True
        )
        results = returned.reshape(experts, capacity, width)[chosen, slots]
        results = results.reshape(tok_rows, top_count, width).astype(jnp.float32)
        weights = probs / jnp.sum(probs, axis=-1, keepdims=True)
        mixed = jnp.einsum("tk,tkd->td", weights, results)
        return (floated + mixed).astype(jnp.bfloat16)

    def advance(step, carry):
        received, saved = carry
        index = step - section
        valid = jnp.logical_and(index >= 0, index < micro)
        clipped = jnp.clip(index, 0, micro - 1)
        first = lax.dynamic_index_in_dim(hidden_in, clipped, 0, keepdims=False)
        state = jnp.where(section == 0, first, received)
        updated = layer(state, clipped)
        saved = jnp.where(valid, lax.dynamic_update_index_in_dim(saved, updated, clipped, 0), saved)
        received = passed_along(updated, "pipe", 1)
        return (received, saved)

    start = (
        jnp.zeros((tok_rows, width), jnp.bfloat16),
        jnp.zeros((micro, tok_rows, width), jnp.bfloat16),
    )
    received, saved = lax.fori_loop(0, micro + lax.axis_size("pipe") - 1, advance, start)
    return saved[None]


def solution(mesh):
    in_specs = (
        P(None, ("exp", "pair"), None),
        P("pipe", None, ("exp", "pair"), None),
        P("pipe", None, ("exp", "pair"), None),
        P("pipe", None),
        P("pipe", ("exp", "pair"), None, None),
        P("pipe", ("exp", "pair"), None, None),
        P("pipe", ("exp", "pair"), None, None),
    )
    out_specs = P("pipe", None, ("exp", "pair"), None)
    return jax.shard_map(
        on_device, mesh=mesh, in_specs=in_specs, out_specs=out_specs, check_vma=False
    )
```
